32 devices in a mesh: heads: 2 (over x), cp: 16 (over z, y, core).
Axes of the slice: x: 2, y: 2, z: 4, core: 2. Of those that a mesh axis runs over, the one named last changes fastest.
Arguments:
- queries: bfloat16 [12, 128, 52, 128], P(None, 'cp', 'heads'), parts along dimension 2
- key_vecs: bfloat16 [2048, 52, 128], P('cp', 'heads'), parts along dimension 1
- value_vecs: bfloat16 [2048, 52, 128], P('cp', 'heads'), parts along dimension 1
- attn_out: bfloat16 [12, 128, 52, 128], P(None, 'cp', 'heads'), parts along dimension 2
- log_sum_exp: float32 [12, 128, 52], P(None, 'cp', 'heads'), parts along dimension 2
- grad_out: bfloat16 [12, 128, 52, 128], P(None, 'cp', 'heads'), parts along dimension 2
Outputs:
- output 1: bfloat16 [12, 128, 52, 128], P(None, 'cp', 'heads'), parts along dimension 2
- output 2: float32 [2048, 52, 128], P('cp', 'heads'), parts along dimension 1
- output 3: float32 [2048, 52, 128], P('cp', 'heads'), parts along dimension 1
There are 2 independent parts. The reference program is written for one: setup_inputs(seed, part) draws one part's arguments, and reference() takes and returns one part's arrays. A program takes and returns all parts, laid end to end along the dimension named above; each array names one.
All inputs are finite; a program needn't handle non-finite values.
Results may differ from the reference program's by a relative error of at most 0.001.
Values are sent between devices in bfloat16 or wider.
A program may use at most 1 GiB of HBM per device.

```python
import jax
import jax.numpy as jnp
from jax import lax

SEGMENTS = 12
BLOCKS = 16
SEG_BLOCK = 8
KEY_BLOCK = 128
HEADS_PART = 26
HEAD_DIM = 128

SEG_LEN = BLOCKS * SEG_BLOCK
PREFIX = BLOCKS * KEY_BLOCK
PREFIX0 = PREFIX - SEGMENTS * SEG_LEN
N_QBLOCKS = SEGMENTS * BLOCKS
SCORE_SCALE = HEAD_DIM ** -0.5


def forward_all(queries, key_vecs, value_vecs):
    tile_shape = (BLOCKS, KEY_BLOCK, HEADS_PART, HEAD_DIM)
    key_tiles = key_vecs.astype(jnp.float32).reshape(tile_shape)
    value_tiles = value_vecs.astype(jnp.float32).reshape(tile_shape)
    tile_starts = KEY_BLOCK * jnp.arange(BLOCKS)
    q_blocks = queries.astype(jnp.float32).reshape(N_QBLOCKS, SEG_BLOCK, HEADS_PART, HEAD_DIM)
    q_starts = PREFIX0 + SEG_BLOCK * jnp.arange(N_QBLOCKS)

    def one_block(block_in):
        q_blk, q_start = block_in
        q_pos = q_start + jnp.arange(SEG_BLOCK)

        def key_step(state_in, tile_in):
            run_max, run_sum, acc_out = state_in
            k_tile, v_tile, k_start = tile_in
            k_pos = k_start + jnp.arange(KEY_BLOCK)
            causal = (q_pos[:, None] >= k_pos[None, :])[None]
            scores = jnp.einsum("qhd,khd->hqk", q_blk, k_tile) * SCORE_SCALE
            scores = jnp.where(causal, scores, -1e30)
            new_max = jnp.maximum(run_max, jnp.max(scores, axis=-1))
            rescale = jnp.exp(run_max - new_max)
            weights = jnp.exp(scores - new_max[:, :, None])
            run_sum = run_sum * rescale + jnp.sum(weights, axis=-1)
            acc_out = acc_out * rescale[:, :, None] + jnp.einsum("hqk,khd->hqd", weights, v_tile)
            return (new_max, run_sum, acc_out), None

        init_state = (jnp.full((HEADS_PART, SEG_BLOCK), -1e30, jnp.float32), jnp.zeros((HEADS_PART, SEG_BLOCK), jnp.float32), jnp.zeros((HEADS_PART, SEG_BLOCK, HEAD_DIM), jnp.float32))
        final_state, unused_ys = lax.scan(key_step, init_state, (key_tiles, value_tiles, tile_starts))
        run_max, run_sum, acc_out = final_state
        out_blk = jnp.transpose(acc_out / run_sum[:, :, None], (1, 0, 2))
        lse_blk = (run_max + jnp.log(run_sum)).T
        return out_blk, lse_blk

    out_blocks, lse_blocks = lax.map(one_block, (q_blocks, q_starts))
    return out_blocks.reshape(SEGMENTS, SEG_LEN, HEADS_PART, HEAD_DIM), lse_blocks.reshape(SEGMENTS, SEG_LEN, HEADS_PART)


def setup_inputs(seed: int = 0, part: int = 0) -> dict:
    base_key = jax.random.fold_in(jax.random.key(seed), part)
    key_q, key_k, key_v, key_mean, key_do = jax.random.split(base_key, 5)
    q_shape = (SEGMENTS, SEG_LEN, HEADS_PART, HEAD_DIM)
    kv_shape = (PREFIX, HEADS_PART, HEAD_DIM)
    queries = (1.5 * jax.random.normal(key_q, q_shape, jnp.float32)).astype(jnp.bfloat16)
    key_vecs = jax.random.normal(key_k, kv_shape, jnp.float32).astype(jnp.bfloat16)
    value_mean = jax.random.normal(key_mean, (1, HEADS_PART, HEAD_DIM), jnp.float32)
    value_vecs = (jax.random.normal(key_v, kv_shape, jnp.float32) + value_mean).astype(jnp.bfloat16)
    attn_f32, log_sum_exp = forward_all(queries, key_vecs, value_vecs)
    do_noise = jax.random.normal(key_do, q_shape, jnp.float32)
    grad_out = ((do_noise + 0.5 * attn_f32) * (PREFIX ** 0.5)).astype(jnp.bfloat16)
    return {"queries": queries, "key_vecs": key_vecs, "value_vecs": value_vecs, "attn_out": attn_f32.astype(jnp.bfloat16), "log_sum_exp": log_sum_exp, "grad_out": grad_out}


def reference(queries, key_vecs, value_vecs, attn_out, log_sum_exp, grad_out):
    tile_shape = (BLOCKS, KEY_BLOCK, HEADS_PART, HEAD_DIM)
    key_tiles = key_vecs.astype(jnp.float32).reshape(tile_shape)
    value_tiles = value_vecs.astype(jnp.float32).reshape(tile_shape)
    tile_starts = KEY_BLOCK * jnp.arange(BLOCKS)
    q_shape = (N_QBLOCKS, SEG_BLOCK, HEADS_PART, HEAD_DIM)
    q_blocks = queries.astype(jnp.float32).reshape(q_shape)
    do_blocks = grad_out.astype(jnp.float32).reshape(q_shape)
    row_delta = jnp.sum(grad_out.astype(jnp.float32) * attn_out.astype(jnp.float32), axis=-1)
    delta_blocks = row_delta.reshape(N_QBLOCKS, SEG_BLOCK, HEADS_PART)
    lse_blocks = log_sum_exp.reshape(N_QBLOCKS, SEG_BLOCK, HEADS_PART)
    q_starts = PREFIX0 + SEG_BLOCK * jnp.arange(N_QBLOCKS)

    def query_step(acc_pair, block_in):
        acc_k, acc_v = acc_pair
        q_blk, do_blk, lse_blk, delta_blk, q_start = block_in
        q_pos = q_start + jnp.arange(SEG_BLOCK)
        lse_rows = lse_blk.T[:, :, None]
        delta_rows = delta_blk.T[:, :, None]

        def key_step(dq_acc, tile_in):
            k_tile, v_tile, k_start = tile_in
            k_pos = k_start + jnp.arange(KEY_BLOCK)
            causal = (q_pos[:, None] >= k_pos[None, :])[None]
            scores = jnp.einsum("qhd,khd->hqk", q_blk, k_tile) * SCORE_SCALE
            weights = jnp.where(causal, jnp.exp(scores - lse_rows), 0.0)
            w_bf = weights.astype(jnp.bfloat16).astype(jnp.float32)
            tile_v = jnp.einsum("hqk,qhd->khd", w_bf, do_blk)
            grad_p = jnp.einsum("qhd,khd->hqk", do_blk, v_tile)
            grad_s = (weights * (grad_p - delta_rows)).astype(jnp.bfloat16).astype(jnp.float32)
            dq_acc = dq_acc + jnp.einsum("hqk,khd->qhd", grad_s, k_tile)
            tile_k = jnp.einsum("hqk,qhd->khd", grad_s, q_blk) * SCORE_SCALE
            return dq_acc, (tile_k, tile_v)

        dq_init = jnp.zeros((SEG_BLOCK, HEADS_PART, HEAD_DIM), jnp.float32)
        dq_acc, tile_grads = lax.scan(key_step, dq_init, (key_tiles, value_tiles, tile_starts))
        acc_k = acc_k + tile_grads[0].reshape(PREFIX, HEADS_PART, HEAD_DIM)
        acc_v = acc_v + tile_grads[1].reshape(PREFIX, HEADS_PART, HEAD_DIM)
        return (acc_k, acc_v), (dq_acc * SCORE_SCALE).astype(jnp.bfloat16)

    zero_kv = jnp.zeros((PREFIX, HEADS_PART, HEAD_DIM), jnp.float32)
    kv_grads, dq_blocks = lax.scan(query_step, (zero_kv, zero_kv), (q_blocks, do_blocks, lse_blocks, delta_blocks, q_starts))
    return dq_blocks.reshape(SEGMENTS, SEG_LEN, HEADS_PART, HEAD_DIM), kv_grads[0], kv_grads[1]
```

```python
import functools

import jax
import jax.numpy as jnp
from jax import lax
from jax.experimental import pallas as pl
from jax.experimental.pallas import tpu as pltpu
from jax.sharding import PartitionSpec as P

MESH = pl.DeviceIdType.MESH
N_CP = 16
N_HEADS = 26
N_SLOTS = 2
N_GROUPS = 3
G_ROWS = 32
SEG_PER_G = 4
Q_LOCAL = 8
K_LOCAL = 128
HD = 128
SEG_LEN = N_CP * Q_LOCAL
GROUP_Q = N_CP * G_ROWS
KEY_SUPER = 512
SRC_PER_SUPER = KEY_SUPER // K_LOCAL
N_SUPER = N_CP // SRC_PER_SUPER
PREFIX0 = 512
KEY_TILE = 256


def head_of(slot, dev):
    second = jnp.where(dev % 2 == 0, 16 + dev // 2, jnp.where(dev == 5, 24, 25))
    return jnp.where(slot == 0, dev, second)


def slots_of(dev):
    return jnp.where((dev % 2 == 0) | (dev == 5) | (dev == 11), 2, 1)


def kernel(qd_ref, kv_ref, st_ref, dq_out, dkv_out, q_buf, kv_buf, st_buf, dq_acc, dq_stage, dkv_stage, in_sems, send_sems, ret_sems, out_sems):
    me = lax.axis_index("cp")
    my_slots = slots_of(me)
    score_scale = HD ** -0.5

    barrier = pltpu.get_barrier_semaphore()

    def greet(k, carry):
        pl.semaphore_signal(barrier, inc=1, device_id={"cp": lax.rem(me + k, N_CP)}, device_id_type=MESH)
        return carry

    lax.fori_loop(1, N_CP, greet, 0)
    pl.semaphore_wait(barrier, N_CP - 1)

    def in_parts(slot, head, src):
        return (
            (qd_ref.at[head], q_buf.at[slot, :, :, src]),
            (kv_ref.at[head], kv_buf.at[slot, :, src]),
            (st_ref.at[head], st_buf.at[slot, src]),
        )

    def in_copies(slot, dev):
        head = head_of(slot, dev)
        return [
            pltpu.make_async_remote_copy(
                src_ref=src, dst_ref=dst, send_sem=send_sems.at[slot, kind, dev], recv_sem=in_sems.at[slot, kind],
                device_id={"cp": dev}, device_id_type=MESH,
            )
            for kind, (src, dst) in enumerate(in_parts(slot, head, me))
        ]

    for slot in range(N_SLOTS):

        @pl.when(slot < my_slots)
        def _():
            for kind, (src, dst) in enumerate(in_parts(slot, head_of(slot, me), me)):
                pltpu.make_async_copy(src, dst, in_sems.at[slot, kind]).start()

        def send(k, carry):
            dev = lax.rem(me + k, N_CP)

            @pl.when(slot < slots_of(dev))
            def _():
                for copy in in_copies(slot, dev):
                    copy.start()

            return carry

        lax.fori_loop(1, N_CP, send, 0)

    def dkv_remote(slot, dev):
        return pltpu.make_async_remote_copy(
            src_ref=dkv_stage.at[slot, :, dev], dst_ref=dkv_out.at[head_of(slot, me)], send_sem=ret_sems.at[slot, 1, dev],
            recv_sem=out_sems.at[1], device_id={"cp": dev}, device_id_type=MESH,
        )

    def dq_remote(slot, dev):
        return pltpu.make_async_remote_copy(
            src_ref=dq_stage.at[slot, :, dev], dst_ref=dq_out.at[head_of(slot, me)], send_sem=ret_sems.at[slot, 0, dev],
            recv_sem=out_sems.at[0], device_id={"cp": dev}, device_id_type=MESH,
        )

    key_iota = lax.broadcasted_iota(jnp.int32, (KEY_TILE, GROUP_Q), 0)
    lane = lax.broadcasted_iota(jnp.int32, (1, GROUP_Q), 1)
    lane_pos = PREFIX0 + (lane % G_ROWS // Q_LOCAL) * SEG_LEN + (lane // G_ROWS) * Q_LOCAL + lane % Q_LOCAL

    def run_slot(slot, carry):
        for kind, buf in enumerate((q_buf, kv_buf, st_buf)):
            pltpu.make_async_copy(buf.at[slot], buf.at[slot], in_sems.at[slot, kind]).wait()
        dq_acc[...] = jnp.zeros_like(dq_acc)

        def run_super(sup, carry):
            dkv_stage[slot, :, pl.ds(sup * SRC_PER_SUPER, SRC_PER_SUPER)] = jnp.zeros((2, SRC_PER_SUPER, K_LOCAL, HD), jnp.float32)

            def run_group(grp, carry):
                q = q_buf[slot, 0, grp].reshape(GROUP_Q, HD)
                do = q_buf[slot, 1, grp].reshape(GROUP_Q, HD)
                lse_rows, delta_rows = [], []
                for quad in range(N_CP // 4):
                    lse_rows.append(jnp.sum(st_buf[slot, pl.ds(quad * 4, 4), grp], axis=0, keepdims=True))
                    delta_rows.append(jnp.sum(st_buf[slot, pl.ds(quad * 4, 4), N_GROUPS + grp], axis=0, keepdims=True))
                lse = jnp.concatenate(lse_rows, axis=1)
                delta = jnp.concatenate(delta_rows, axis=1)
                q_pos = lane_pos + grp * (SEG_PER_G * SEG_LEN)
                dq_part = jnp.zeros((GROUP_Q, HD), jnp.float32)
                for tile in range(KEY_SUPER // KEY_TILE):
                    per = KEY_TILE // K_LOCAL
                    block = pl.ds(sup * SRC_PER_SUPER + tile * per, per)
                    key = kv_buf[slot, 0, block].reshape(KEY_TILE, HD)
                    val = kv_buf[slot, 1, block].reshape(KEY_TILE, HD)
                    causal = key_iota + (sup * KEY_SUPER + tile * KEY_TILE) <= q_pos
                    contract_last = (((1,), (1,)), ((), ()))
                    scores = lax.dot_general(key, q, contract_last, preferred_element_type=jnp.float32) * score_scale
                    weights = jnp.where(causal, jnp.exp(scores - lse), 0.0)
                    grad_p = lax.dot_general(val, do, contract_last, preferred_element_type=jnp.float32)
                    grad_s = (weights * (grad_p - delta)).astype(jnp.bfloat16)
                    part_v = jnp.dot(weights.astype(jnp.bfloat16), do, preferred_element_type=jnp.float32)
                    part_k = jnp.dot(grad_s, q, preferred_element_type=jnp.float32)
                    dkv_stage[slot, 0, block] += (part_k * score_scale).reshape(per, K_LOCAL, HD)
                    dkv_stage[slot, 1, block] += part_v.reshape(per, K_LOCAL, HD)
                    dq_part += lax.dot_general(grad_s, key, (((0,), (0,)), ((), ())), preferred_element_type=jnp.float32)
                dq_acc[grp] += dq_part
                return carry

            lax.fori_loop(jnp.maximum(sup - 1, 0), N_GROUPS, run_group, 0)

            def give_back(k, carry):
                dev = sup * SRC_PER_SUPER + k

                @pl.when(dev != me)
                def _():
                    dkv_remote(slot, dev).start()

                @pl.when(dev == me)
                def _():
                    pltpu.make_async_copy(dkv_stage.at[slot, :, me], dkv_out.at[head_of(slot, me)], out_sems.at[1]).start()

                return carry

            lax.fori_loop(0, SRC_PER_SUPER, give_back, 0)
            return carry

        lax.fori_loop(0, N_SUPER, run_super, 0)
        dq_stage[slot] = (dq_acc[...] * score_scale).astype(jnp.bfloat16).reshape(N_GROUPS, N_CP, G_ROWS, HD)
        pltpu.make_async_copy(dq_stage.at[slot, :, me], dq_out.at[head_of(slot, me)], out_sems.at[0]).start()

        def give_dq(k, carry):
            dq_remote(slot, lax.rem(me + k, N_CP)).start()
            return carry

        lax.fori_loop(1, N_CP, give_dq, 0)
        return carry

    lax.fori_loop(0, my_slots, run_slot, 0)

    pltpu.make_async_copy(dq_out, dq_out, out_sems.at[0]).wait()
    pltpu.make_async_copy(dkv_out, dkv_out, out_sems.at[1]).wait()

    for slot in range(N_SLOTS):

        def drain(k, carry):
            dev = lax.rem(me + k, N_CP)

            @pl.when(slot < slots_of(dev))
            def _():
                for copy in in_copies(slot, dev):
                    copy.wait_send()

            @pl.when(slot < my_slots)
            def _():
                dq_remote(slot, dev).wait_send()
                dkv_remote(slot, dev).wait_send()

            return carry

        lax.fori_loop(1, N_CP, drain, 0)


def solution(mesh):
    spec_q = P(None, "cp", "heads", None)
    spec_kv = P("cp", "heads", None)
    spec_lse = P(None, "cp", "heads")

    def per_device(queries, key_vecs, value_vecs, attn_out, log_sum_exp, grad_out):
        rows = queries.shape[0] * queries.shape[1]
        row_delta = jnp.sum(grad_out.astype(jnp.float32) * attn_out.astype(jnp.float32), axis=-1)
        by_head = lambda x: x.reshape(rows, N_HEADS, HD).transpose(1, 0, 2).reshape(N_HEADS, N_GROUPS, G_ROWS, HD)
        qd = jnp.stack([by_head(queries), by_head(grad_out)], axis=1)
        kv = jnp.stack([key_vecs.transpose(1, 0, 2), value_vecs.transpose(1, 0, 2)], axis=1)
        stats = jnp.stack([log_sum_exp, row_delta]).reshape(2, N_GROUPS, G_ROWS, N_HEADS).transpose(3, 0, 1, 2).reshape(N_HEADS, 6, 1, G_ROWS)
        quarter = (jnp.arange(4) == lax.axis_index("cp") % 4)[:, None]
        stats = jnp.where(quarter, stats, 0.0).reshape(N_HEADS, 6, 4 * G_ROWS)
        stats = jnp.pad(stats, ((0, 0), (0, 2), (0, 0)))

        any_spec = pl.BlockSpec(memory_space=pl.ANY)
        dq, dkv = pl.pallas_call(
            kernel,
            out_shape=(
                jax.ShapeDtypeStruct((N_HEADS, N_GROUPS, G_ROWS, HD), jnp.bfloat16),
                jax.ShapeDtypeStruct((N_HEADS, 2, K_LOCAL, HD), jnp.float32),
            ),
            in_specs=[any_spec] * 3,
            out_specs=(any_spec, any_spec),
            scratch_shapes=[
                pltpu.VMEM((N_SLOTS, 2, N_GROUPS, N_CP, G_ROWS, HD), jnp.bfloat16),
                pltpu.VMEM((N_SLOTS, 2, N_CP, K_LOCAL, HD), jnp.bfloat16),
                pltpu.VMEM((N_SLOTS, N_CP, 8, 128), jnp.float32),
                pltpu.VMEM((N_GROUPS, GROUP_Q, HD), jnp.float32),
                pltpu.VMEM((N_SLOTS, N_GROUPS, N_CP, G_ROWS, HD), jnp.bfloat16),
                pltpu.VMEM((N_SLOTS, 2, N_CP, K_LOCAL, HD), jnp.float32),
                pltpu.SemaphoreType.DMA((N_SLOTS, 3)),
                pltpu.SemaphoreType.DMA((N_SLOTS, 3, N_CP)),
                pltpu.SemaphoreType.DMA((N_SLOTS, 2, N_CP)),
                pltpu.SemaphoreType.DMA((2,)),
            ],
            compiler_params=pltpu.CompilerParams(collective_id=0, has_side_effects=True, vmem_limit_bytes=40 * 1024 * 1024),
            name="head_exchange",
        )(qd, kv, stats)

        dq = dq.reshape(N_HEADS, rows, HD).transpose(1, 0, 2).reshape(queries.shape)
        return dq, dkv[:, 0].transpose(1, 0, 2), dkv[:, 1].transpose(1, 0, 2)

    return jax.shard_map(per_device, mesh=mesh, in_specs=(spec_q, spec_kv, spec_kv, spec_q, spec_lse, spec_q), out_specs=(spec_q, spec_kv, spec_kv), check_vma=False)
```

```python
import functools

import jax
import jax.numpy as jnp
from jax import lax
from jax.experimental import pallas as pl
from jax.experimental.pallas import tpu as pltpu
from jax.sharding import PartitionSpec as P

MESH = pl.DeviceIdType.MESH
N_CP = 16
N_HEADS = 26
N_HALF = 8
N_SLOTS = 5
N_GROUPS = 3
G_ROWS = 32
SEG_PER_G = 4
Q_LOCAL = 8
K_LOCAL = 128
HD = 128
SEG_LEN = N_CP * Q_LOCAL
GROUP_Q = N_CP * G_ROWS
KEY_SUPER = 512
SRC_PER_SUPER = KEY_SUPER // K_LOCAL
SUPER_PER_HALF = N_HALF // SRC_PER_SUPER
PREFIX0 = 512
KEY_TILE = 256


def at_end(dev):
    return (dev < 4) | (dev >= 12)


def head_of(slot, dev):
    return jnp.where(at_end(dev), 19 + 3 * slot, 4 * slot) + dev % 4


def slots_of(dev):
    pos = dev % 4
    return jnp.where(at_end(dev), jnp.where(pos >= 1, 2, 1), jnp.where(pos <= 2, 5, 4))


def kernel(qd_ref, kv_ref, st_ref, dq_out, dkv_out, q_buf, kv_buf, st_buf, part_buf, dq_acc, dq_stage, dkv_stage, in_sems, send_sems, ret_sems, part_sems, out_sems):
    me = lax.axis_index("cp")
    my_slots = slots_of(me)
    half = me // N_HALF
    half_dev = half * N_HALF
    partner = (3 - me // 4) * 4 + me % 4
    score_scale = HD ** -0.5

    barrier = pltpu.get_barrier_semaphore()

    def greet(k, carry):
        pl.semaphore_signal(barrier, inc=1, device_id={"cp": lax.rem(me + k, N_CP)}, device_id_type=MESH)
        return carry

    lax.fori_loop(1, N_CP, greet, 0)
    pl.semaphore_wait(barrier, N_CP - 1)

    def in_parts(slot, dev, dev_half):
        head = head_of(slot, dev)
        first = dev_half
        q_part = (0, qd_ref.at[head, :, first:], q_buf.at[slot, :, first:, me])
        kv_part = (1, kv_ref.at[head], kv_buf.at[slot, :, me % N_HALF])
        st_part = (2, st_ref.at[head], st_buf.at[slot, me])
        return q_part, kv_part, st_part

    def in_remote(slot, dev, part):
        kind, src, dst = part
        return pltpu.make_async_remote_copy(
            src_ref=src, dst_ref=dst, send_sem=send_sems.at[slot, kind, dev], recv_sem=in_sems.at[slot, kind],
            device_id={"cp": dev}, device_id_type=MESH,
        )

    def each_in_copy(slot, dev, act):
        for dev_half in range(2):

            @pl.when((slot < slots_of(dev)) & (dev // N_HALF == dev_half))
            def _():
                q_part, kv_part, st_part = in_parts(slot, dev, dev_half)
                act(in_remote(slot, dev, st_part))
                act(in_remote(slot, dev, q_part))

                @pl.when(half == dev_half)
                def _():
                    act(in_remote(slot, dev, kv_part))

    for slot in range(N_SLOTS):
        for my_half in range(2):

            @pl.when((slot < my_slots) & (half == my_half))
            def _():
                for kind, src, dst in in_parts(slot, me, my_half):
                    pltpu.make_async_copy(src, dst, in_sems.at[slot, kind]).start()

        def send(k, carry):
            each_in_copy(slot, lax.rem(me + k, N_CP), lambda copy: copy.start())
            return carry

        lax.fori_loop(1, N_CP, send, 0)

    def dkv_remote(slot, dev):
        return pltpu.make_async_remote_copy(
            src_ref=dkv_stage.at[slot, :, dev % N_HALF], dst_ref=dkv_out.at[head_of(slot, me)], send_sem=ret_sems.at[slot, 1, dev % N_HALF],
            recv_sem=out_sems.at[1], device_id={"cp": dev}, device_id_type=MESH,
        )

    def dq_remote(slot, dev):
        return pltpu.make_async_remote_copy(
            src_ref=dq_stage.at[slot, :, dev % N_HALF], dst_ref=dq_out.at[head_of(slot, me)], send_sem=ret_sems.at[slot, 0, dev % N_HALF],
            recv_sem=out_sems.at[0], device_id={"cp": dev}, device_id_type=MESH,
        )

    def part_remote(slot, my_half):
        first, other = my_half, (1 - my_half) * N_HALF
        return pltpu.make_async_remote_copy(
            src_ref=dq_acc.at[slot, first:, other:other + N_HALF], dst_ref=part_buf.at[slot, first:], send_sem=part_sems.at[0, slot],
            recv_sem=part_sems.at[1, slot], device_id={"cp": partner}, device_id_type=MESH,
        )

    key_iota = lax.broadcasted_iota(jnp.int32, (KEY_TILE, GROUP_Q), 0)
    lane = lax.broadcasted_iota(jnp.int32, (1, GROUP_Q), 1)
    lane_pos = PREFIX0 + (lane % G_ROWS // Q_LOCAL) * SEG_LEN + (lane // G_ROWS) * Q_LOCAL + lane % Q_LOCAL

    def finish_dq(slot):
        for my_half in range(2):

            @pl.when(half == my_half)
            def _():
                arrived = part_buf.at[slot, 1 - my_half:]
                pltpu.make_async_copy(arrived, arrived, part_sems.at[1, slot]).wait()
                own = pl.ds(my_half * N_HALF, N_HALF)
                first = dq_acc[slot, 0, own] if my_half == 0 else part_buf[slot, 0]
                dq_stage[slot, 0] = (first * score_scale).astype(jnp.bfloat16)
                for grp in range(1, N_GROUPS):
                    dq_stage[slot, grp] = ((dq_acc[slot, grp, own] + part_buf[slot, grp]) * score_scale).astype(jnp.bfloat16)

        pltpu.make_async_copy(dq_stage.at[slot, :, me % N_HALF], dq_out.at[head_of(slot, me)], out_sems.at[0]).start()

        def give_dq(k, carry):
            dq_remote(slot, half_dev + lax.rem(me + k, N_HALF)).start()
            return carry

        lax.fori_loop(1, N_HALF, give_dq, 0)

    def run_slot(slot, carry):
        for my_half in range(2):

            @pl.when(half == my_half)
            def _():
                arrived = q_buf.at[slot, :, my_half:]
                pltpu.make_async_copy(arrived, arrived, in_sems.at[slot, 0]).wait()

        for kind, buf in ((1, kv_buf), (2, st_buf)):
            pltpu.make_async_copy(buf.at[slot], buf.at[slot], in_sems.at[slot, kind]).wait()
        dq_acc[slot] = jnp.zeros(dq_acc.shape[1:], jnp.float32)

        def run_super(sup_local, carry):
            sup = half * SUPER_PER_HALF + sup_local
            dkv_stage[slot, :, pl.ds(sup_local * SRC_PER_SUPER, SRC_PER_SUPER)] = jnp.zeros((2, SRC_PER_SUPER, K_LOCAL, HD), jnp.float32)

            def run_group(grp, carry):
                q = q_buf[slot, 0, grp].reshape(GROUP_Q, HD)
                do = q_buf[slot, 1, grp].reshape(GROUP_Q, HD)
                lse_rows, delta_rows = [], []
                for quad in range(N_CP // 4):
                    lse_rows.append(jnp.sum(st_buf[slot, pl.ds(quad * 4, 4), grp], axis=0, keepdims=True))
                    delta_rows.append(jnp.sum(st_buf[slot, pl.ds(quad * 4, 4), N_GROUPS + grp], axis=0, keepdims=True))
                lse = jnp.concatenate(lse_rows, axis=1)
                delta = jnp.concatenate(delta_rows, axis=1)
                q_pos = lane_pos + grp * (SEG_PER_G * SEG_LEN)
                dq_part = jnp.zeros((GROUP_Q, HD), jnp.float32)
                for tile in range(KEY_SUPER // KEY_TILE):
                    per = KEY_TILE // K_LOCAL
                    block = pl.ds(sup_local * SRC_PER_SUPER + tile * per, per)
                    key = kv_buf[slot, 0, block].reshape(KEY_TILE, HD)
                    val = kv_buf[slot, 1, block].reshape(KEY_TILE, HD)
                    causal = key_iota + (sup * KEY_SUPER + tile * KEY_TILE) <= q_pos
                    contract_last = (((1,), (1,)), ((), ()))
                    scores = lax.dot_general(key, q, contract_last, preferred_element_type=jnp.float32) * score_scale
                    weights = jnp.where(causal, jnp.exp(scores - lse), 0.0)
                    grad_p = lax.dot_general(val, do, contract_last, preferred_element_type=jnp.float32)
                    grad_s = (weights * (grad_p - delta)).astype(jnp.bfloat16)
                    part_v = jnp.dot(weights.astype(jnp.bfloat16), do, preferred_element_type=jnp.float32)
                    part_k = jnp.dot(grad_s, q, preferred_element_type=jnp.float32)
                    dkv_stage[slot, 0, block] += (part_k * score_scale).reshape(per, K_LOCAL, HD)
                    dkv_stage[slot, 1, block] += part_v.reshape(per, K_LOCAL, HD)
                    dq_part += lax.dot_general(grad_s, key, (((0,), (0,)), ((), ())), preferred_element_type=jnp.float32)
                dq_acc[slot, grp] += dq_part.reshape(N_CP, G_ROWS, HD)
                return carry

            lax.fori_loop(jnp.maximum(sup - 1, 0), N_GROUPS, run_group, 0)

            def give_back(k, carry):
                dev = half_dev + sup_local * SRC_PER_SUPER + k

                @pl.when(dev != me)
                def _():
                    dkv_remote(slot, dev).start()

                @pl.when(dev == me)
                def _():
                    pltpu.make_async_copy(dkv_stage.at[slot, :, me % N_HALF], dkv_out.at[head_of(slot, me)], out_sems.at[1]).start()

                return carry

            lax.fori_loop(0, SRC_PER_SUPER, give_back, 0)
            return carry

        lax.fori_loop(0, SUPER_PER_HALF, run_super, 0)
        for my_half in range(2):

            @pl.when(half == my_half)
            def _():
                part_remote(slot, my_half).start()

        @pl.when(slot > 0)
        def _():
            finish_dq(slot - 1)

        return carry

    lax.fori_loop(0, my_slots, run_slot, 0)
    finish_dq(my_slots - 1)

    pltpu.make_async_copy(dq_out, dq_out, out_sems.at[0]).wait()
    pltpu.make_async_copy(dkv_out, dkv_out, out_sems.at[1]).wait()

    for slot in range(N_SLOTS):

        def drain(k, carry):
            each_in_copy(slot, lax.rem(me + k, N_CP), lambda copy: copy.wait_send())
            return carry

        lax.fori_loop(1, N_CP, drain, 0)

        @pl.when(slot < my_slots)
        def _():
            def drain_back(k, carry):
                dev = half_dev + lax.rem(me + k, N_HALF)
                dq_remote(slot, dev).wait_send()
                dkv_remote(slot, dev).wait_send()
                return carry

            lax.fori_loop(1, N_HALF, drain_back, 0)
            for my_half in range(2):

                @pl.when(half == my_half)
                def _():
                    part_remote(slot, my_half).wait_send()


def solution(mesh):
    spec_q = P(None, "cp", "heads", None)
    spec_kv = P("cp", "heads", None)
    spec_lse = P(None, "cp", "heads")

    def per_device(queries, key_vecs, value_vecs, attn_out, log_sum_exp, grad_out):
        rows = queries.shape[0] * queries.shape[1]
        row_delta = jnp.sum(grad_out.astype(jnp.float32) * attn_out.astype(jnp.float32), axis=-1)
        by_head = lambda x: x.reshape(rows, N_HEADS, HD).transpose(1, 0, 2).reshape(N_HEADS, N_GROUPS, G_ROWS, HD)
        qd = jnp.stack([by_head(queries), by_head(grad_out)], axis=1)
        kv = jnp.stack([key_vecs.transpose(1, 0, 2), value_vecs.transpose(1, 0, 2)], axis=1)
        stats = jnp.stack([log_sum_exp, row_delta]).reshape(2, N_GROUPS, G_ROWS, N_HEADS).transpose(3, 0, 1, 2).reshape(N_HEADS, 6, 1, G_ROWS)
        quarter = (jnp.arange(4) == lax.axis_index("cp") % 4)[:, None]
        stats = jnp.where(quarter, stats, 0.0).reshape(N_HEADS, 6, 4 * G_ROWS)
        stats = jnp.pad(stats, ((0, 0), (0, 2), (0, 0)))

        any_spec = pl.BlockSpec(memory_space=pl.ANY)
        dq, dkv = pl.pallas_call(
            kernel,
            out_shape=(
                jax.ShapeDtypeStruct((N_HEADS, N_GROUPS, G_ROWS, HD), jnp.bfloat16),
                jax.ShapeDtypeStruct((N_HEADS, 2, K_LOCAL, HD), jnp.float32),
            ),
            in_specs=[any_spec] * 3,
            out_specs=(any_spec, any_spec),
            scratch_shapes=[
                pltpu.VMEM((N_SLOTS, 2, N_GROUPS, N_CP, G_ROWS, HD), jnp.bfloat16),
                pltpu.VMEM((N_SLOTS, 2, N_HALF, K_LOCAL, HD), jnp.bfloat16),
                pltpu.VMEM((N_SLOTS, N_CP, 8, 128), jnp.float32),
                pltpu.VMEM((N_SLOTS, N_GROUPS, N_HALF, G_ROWS, HD), jnp.float32),
                pltpu.VMEM((N_SLOTS, N_GROUPS, N_CP, G_ROWS, HD), jnp.float32),
                pltpu.VMEM((N_SLOTS, N_GROUPS, N_HALF, G_ROWS, HD), jnp.bfloat16),
                pltpu.VMEM((N_SLOTS, 2, N_HALF, K_LOCAL, HD), jnp.float32),
                pltpu.SemaphoreType.DMA((N_SLOTS, 3)),
                pltpu.SemaphoreType.DMA((N_SLOTS, 3, N_CP)),
                pltpu.SemaphoreType.DMA((N_SLOTS, 2, N_HALF)),
                pltpu.SemaphoreType.DMA((2, N_SLOTS)),
                pltpu.SemaphoreType.DMA((2,)),
            ],
            compiler_params=pltpu.CompilerParams(collective_id=0, has_side_effects=True, vmem_limit_bytes=40 * 1024 * 1024),
            name="head_exchange",
        )(qd, kv, stats)

        dq = dq.reshape(N_HEADS, rows, HD).transpose(1, 0, 2).reshape(queries.shape)
        return dq, dkv[:, 0].transpose(1, 0, 2), dkv[:, 1].transpose(1, 0, 2)

    return jax.shard_map(per_device, mesh=mesh, in_specs=(spec_q, spec_kv, spec_kv, spec_q, spec_lse, spec_q), out_specs=(spec_q, spec_kv, spec_kv), check_vma=False)
```

```python
import functools

import jax
import jax.numpy as jnp
from jax import lax
from jax.experimental import pallas as pl
from jax.experimental.pallas import tpu as pltpu
from jax.sharding import PartitionSpec as P

MESH = pl.DeviceIdType.MESH
N_CP = 16
N_HEADS = 26
N_HALF = 8
N_SLOTS = 6
N_GROUPS = 3
G_ROWS = 32
SEG_PER_G = 4
Q_LOCAL = 8
K_LOCAL = 128
HD = 128
SEG_LEN = N_CP * Q_LOCAL
GROUP_Q = N_CP * G_ROWS
KEY_SUPER = 512
SRC_PER_SUPER = KEY_SUPER // K_LOCAL
SUPER_PER_HALF = N_HALF // SRC_PER_SUPER
PREFIX0 = 512
KEY_TILE = 256


def at_end(dev):
    return (dev < 4) | (dev >= 12)


def head_of(slot, dev):
    pos = dev % 4
    return jnp.where(at_end(dev), 22 + pos, jnp.where(slot == 5, 20 + pos // 2, 4 * slot + pos))


def slots_of(dev):
    return jnp.where(at_end(dev), 1, jnp.where(dev % 2 == 0, 6, 5))


def kernel(qd_ref, kv_ref, st_ref, dq_out, dkv_out, q_buf, kv_buf, st_buf, part_buf, dq_acc, dq_stage, dkv_stage, in_sems, send_sems, direct_sems, fwd_sems, ret_sems, part_sems, out_sems):
    me = lax.axis_index("cp")
    my_slots = slots_of(me)
    half = me // N_HALF
    half_dev = half * N_HALF
    partner = (3 - me // 4) * 4 + me % 4
    score_scale = HD ** -0.5

    barrier = pltpu.get_barrier_semaphore()

    def greet(k, carry):
        pl.semaphore_signal(barrier, inc=1, device_id={"cp": lax.rem(me + k, N_CP)}, device_id_type=MESH)
        return carry

    lax.fori_loop(1, N_CP, greet, 0)
    pl.semaphore_wait(barrier, N_CP - 1)

    def in_parts(slot, dev):
        head = head_of(slot, dev)
        return (
            (0, qd_ref.at[head], q_buf.at[slot, :, :, me]),
            (1, kv_ref.at[head], kv_buf.at[slot, :, me % N_HALF]),
            (2, st_ref.at[head], st_buf.at[slot, me]),
        )

    def each_in_copy(slot, act):
        def one(k, carry):
            dev = half_dev + lax.rem(me + k, N_HALF)

            @pl.when(slot < slots_of(dev))
            def _():
                for kind, src, dst in in_parts(slot, dev):
                    act(pltpu.make_async_remote_copy(
                        src_ref=src, dst_ref=dst, send_sem=send_sems.at[slot, kind, dev % N_HALF], recv_sem=in_sems.at[slot, kind],
                        device_id={"cp": dev}, device_id_type=MESH,
                    ))

            return carry

        lax.fori_loop(1, N_HALF, one, 0)

    def each_direct_copy(act):
        for my_half in range(2):

            @pl.when(half == my_half)
            def _():
                first = 1 - my_half

                def one(k, carry):
                    dev = (1 - my_half) * N_HALF + lax.rem(me + k, N_HALF)
                    head = head_of(0, dev)
                    parts = ((qd_ref.at[head, :, first:], q_buf.at[0, :, first:, me]), (st_ref.at[head], st_buf.at[0, me]))
                    for kind, (src, dst) in enumerate(parts):
                        act(pltpu.make_async_remote_copy(
                            src_ref=src, dst_ref=dst, send_sem=direct_sems.at[kind, dev % N_HALF], recv_sem=fwd_sems.at[1, 0, kind],
                            device_id={"cp": dev}, device_id_type=MESH,
                        ))
                    return carry

                lax.fori_loop(0, N_HALF, one, 0)

    for slot in range(N_SLOTS):

        @pl.when(slot < my_slots)
        def _():
            for kind, src, dst in in_parts(slot, me):
                pltpu.make_async_copy(src, dst, in_sems.at[slot, kind]).start()

        if slot == 0:
            each_direct_copy(lambda copy: copy.start())
        each_in_copy(slot, lambda copy: copy.start())

    def slab(slot, of_half):
        first = 1 - of_half
        return q_buf.at[slot, :, first:, of_half * N_HALF:(of_half + 1) * N_HALF]

    def stat_slab(slot, of_half):
        return st_buf.at[slot, of_half * N_HALF:(of_half + 1) * N_HALF]

    def forwards(slot, my_half):
        return [
            pltpu.make_async_remote_copy(
                src_ref=ref, dst_ref=ref, send_sem=fwd_sems.at[0, slot, kind], recv_sem=fwd_sems.at[1, slot, kind],
                device_id={"cp": partner}, device_id_type=MESH,
            )
            for kind, ref in enumerate((slab(slot, my_half), stat_slab(slot, my_half)))
        ]

    def receive(slot):
        own = pl.ds(half_dev, N_HALF)
        for kind, ref in enumerate((q_buf.at[slot, :, :, own], kv_buf.at[slot], st_buf.at[slot, own])):
            pltpu.make_async_copy(ref, ref, in_sems.at[slot, kind]).wait()
        for my_half in range(2):

            @pl.when((half == my_half) & (slot > 0))
            def _():
                for copy in forwards(slot, my_half):
                    copy.start()

    def receive_forwarded(slot):
        for my_half in range(2):

            @pl.when(half == my_half)
            def _():
                for kind, ref in enumerate((slab(slot, 1 - my_half), stat_slab(slot, 1 - my_half))):
                    pltpu.make_async_copy(ref, ref, fwd_sems.at[1, slot, kind]).wait()

    def dkv_remote(slot, dev):
        return pltpu.make_async_remote_copy(
            src_ref=dkv_stage.at[slot, :, dev % N_HALF], dst_ref=dkv_out.at[head_of(slot, me)], send_sem=ret_sems.at[slot, 1, dev % N_HALF],
            recv_sem=out_sems.at[1], device_id={"cp": dev}, device_id_type=MESH,
        )

    def dq_remote(slot, dev):
        return pltpu.make_async_remote_copy(
            src_ref=dq_stage.at[slot, :, dev % N_HALF], dst_ref=dq_out.at[head_of(slot, me)], send_sem=ret_sems.at[slot, 0, dev % N_HALF],
            recv_sem=out_sems.at[0], device_id={"cp": dev}, device_id_type=MESH,
        )

    def part_remote(slot, my_half):
        first, other = my_half, (1 - my_half) * N_HALF
        return pltpu.make_async_remote_copy(
            src_ref=dq_acc.at[slot, first:, other:other + N_HALF], dst_ref=part_buf.at[slot, first:], send_sem=part_sems.at[0, slot],
            recv_sem=part_sems.at[1, slot], device_id={"cp": partner}, device_id_type=MESH,
        )

    key_iota = lax.broadcasted_iota(jnp.int32, (KEY_TILE, GROUP_Q), 0)
    lane = lax.broadcasted_iota(jnp.int32, (1, GROUP_Q), 1)
    lane_pos = PREFIX0 + (lane % G_ROWS // Q_LOCAL) * SEG_LEN + (lane // G_ROWS) * Q_LOCAL + lane % Q_LOCAL

    def finish_dq(slot):
        for my_half in range(2):

            @pl.when(half == my_half)
            def _():
                arrived = part_buf.at[slot, 1 - my_half:]
                pltpu.make_async_copy(arrived, arrived, part_sems.at[1, slot]).wait()
                own = pl.ds(my_half * N_HALF, N_HALF)
                first = dq_acc[slot, 0, own] if my_half == 0 else part_buf[slot, 0]
                dq_stage[slot, 0] = (first * score_scale).astype(jnp.bfloat16)
                for grp in range(1, N_GROUPS):
                    dq_stage[slot, grp] = ((dq_acc[slot, grp, own] + part_buf[slot, grp]) * score_scale).astype(jnp.bfloat16)

        pltpu.make_async_copy(dq_stage.at[slot, :, me % N_HALF], dq_out.at[head_of(slot, me)], out_sems.at[0]).start()

        def give_dq(k, carry):
            dq_remote(slot, half_dev + lax.rem(me + k, N_HALF)).start()
            return carry

        lax.fori_loop(1, N_HALF, give_dq, 0)

    def run_slot(slot, carry):
        @pl.when((slot > 0) & (slot + 1 < my_slots))
        def _():
            receive(slot + 1)

        receive_forwarded(slot)
        dq_acc[slot] = jnp.zeros(dq_acc.shape[1:], jnp.float32)

        def run_super(sup_local, carry):
            sup = half * SUPER_PER_HALF + sup_local
            dkv_stage[slot, :, pl.ds(sup_local * SRC_PER_SUPER, SRC_PER_SUPER)] = jnp.zeros((2, SRC_PER_SUPER, K_LOCAL, HD), jnp.float32)

            def run_group(grp, carry):
                q = q_buf[slot, 0, grp].reshape(GROUP_Q, HD)
                do = q_buf[slot, 1, grp].reshape(GROUP_Q, HD)
                lse_rows, delta_rows = [], []
                for quad in range(N_CP // 4):
                    lse_rows.append(jnp.sum(st_buf[slot, pl.ds(quad * 4, 4), grp], axis=0, keepdims=True))
                    delta_rows.append(jnp.sum(st_buf[slot, pl.ds(quad * 4, 4), N_GROUPS + grp], axis=0, keepdims=True))
                lse = jnp.concatenate(lse_rows, axis=1)
                delta = jnp.concatenate(delta_rows, axis=1)
                q_pos = lane_pos + grp * (SEG_PER_G * SEG_LEN)
                dq_part = jnp.zeros((GROUP_Q, HD), jnp.float32)
                for tile in range(KEY_SUPER // KEY_TILE):
                    per = KEY_TILE // K_LOCAL
                    block = pl.ds(sup_local * SRC_PER_SUPER + tile * per, per)
                    key = kv_buf[slot, 0, block].reshape(KEY_TILE, HD)
                    val = kv_buf[slot, 1, block].reshape(KEY_TILE, HD)
                    causal = key_iota + (sup * KEY_SUPER + tile * KEY_TILE) <= q_pos
                    contract_last = (((1,), (1,)), ((), ()))
                    scores = lax.dot_general(key, q, contract_last, preferred_element_type=jnp.float32) * score_scale
                    weights = jnp.where(causal, jnp.exp(scores - lse), 0.0)
                    grad_p = lax.dot_general(val, do, contract_last, preferred_element_type=jnp.float32)
                    grad_s = (weights * (grad_p - delta)).astype(jnp.bfloat16)
                    part_v = jnp.dot(weights.astype(jnp.bfloat16), do, preferred_element_type=jnp.float32)
                    part_k = jnp.dot(grad_s, q, preferred_element_type=jnp.float32)
                    dkv_stage[slot, 0, block] += (part_k * score_scale).reshape(per, K_LOCAL, HD)
                    dkv_stage[slot, 1, block] += part_v.reshape(per, K_LOCAL, HD)
                    dq_part += lax.dot_general(grad_s, key, (((0,), (0,)), ((), ())), preferred_element_type=jnp.float32)
                dq_acc[slot, grp] += dq_part.reshape(N_CP, G_ROWS, HD)
                return carry

            lax.fori_loop(jnp.maximum(sup - 1, 0), N_GROUPS, run_group, 0)

            def give_back(k, carry):
                dev = half_dev + sup_local * SRC_PER_SUPER + k

                @pl.when(dev != me)
                def _():
                    dkv_remote(slot, dev).start()

                @pl.when(dev == me)
                def _():
                    pltpu.make_async_copy(dkv_stage.at[slot, :, me % N_HALF], dkv_out.at[head_of(slot, me)], out_sems.at[1]).start()

                return carry

            lax.fori_loop(0, SRC_PER_SUPER, give_back, 0)
            return carry

        lax.fori_loop(0, SUPER_PER_HALF, run_super, 0)
        for my_half in range(2):

            @pl.when(half == my_half)
            def _():
                part_remote(slot, my_half).start()

        @pl.when((slot == 0) & (my_slots > 1))
        def _():
            receive(slot + 1)

        @pl.when(slot > 0)
        def _():
            finish_dq(slot - 1)

        return carry

    receive(0)
    lax.fori_loop(0, my_slots, run_slot, 0)
    finish_dq(my_slots - 1)

    for slot in range(N_SLOTS):
        each_in_copy(slot, lambda copy: copy.wait_send())
        if slot == 0:
            each_direct_copy(lambda copy: copy.wait_send())

        @pl.when(slot < my_slots)
        def _():
            def drain(k, carry):
                dev = half_dev + lax.rem(me + k, N_HALF)
                dq_remote(slot, dev).wait_send()
                dkv_remote(slot, dev).wait_send()
                return carry

            lax.fori_loop(1, N_HALF, drain, 0)
            for my_half in range(2):

                @pl.when(half == my_half)
                def _():
                    if slot > 0:
                        for copy in forwards(slot, my_half):
                            copy.wait_send()
                    part_remote(slot, my_half).wait_send()

    pltpu.make_async_copy(dq_out, dq_out, out_sems.at[0]).wait()
    pltpu.make_async_copy(dkv_out, dkv_out, out_sems.at[1]).wait()


def solution(mesh):
    spec_q = P(None, "cp", "heads", None)
    spec_kv = P("cp", "heads", None)
    spec_lse = P(None, "cp", "heads")

    def per_device(queries, key_vecs, value_vecs, attn_out, log_sum_exp, grad_out):
        rows = queries.shape[0] * queries.shape[1]
        row_delta = jnp.sum(grad_out.astype(jnp.float32) * attn_out.astype(jnp.float32), axis=-1)
        by_head = lambda x: x.reshape(rows, N_HEADS, HD).transpose(1, 0, 2).reshape(N_HEADS, N_GROUPS, G_ROWS, HD)
        qd = jnp.stack([by_head(queries), by_head(grad_out)], axis=1)
        kv = jnp.stack([key_vecs.transpose(1, 0, 2), value_vecs.transpose(1, 0, 2)], axis=1)
        stats = jnp.stack([log_sum_exp, row_delta]).reshape(2, N_GROUPS, G_ROWS, N_HEADS).transpose(3, 0, 1, 2).reshape(N_HEADS, 6, 1, G_ROWS)
        quarter = (jnp.arange(4) == lax.axis_index("cp") % 4)[:, None]
        stats = jnp.where(quarter, stats, 0.0).reshape(N_HEADS, 6, 4 * G_ROWS)
        stats = jnp.pad(stats, ((0, 0), (0, 2), (0, 0)))

        any_spec = pl.BlockSpec(memory_space=pl.ANY)
        dq, dkv = pl.pallas_call(
            kernel,
            out_shape=(
                jax.ShapeDtypeStruct((N_HEADS, N_GROUPS, G_ROWS, HD), jnp.bfloat16),
                jax.ShapeDtypeStruct((N_HEADS, 2, K_LOCAL, HD), jnp.float32),
            ),
            in_specs=[any_spec] * 3,
            out_specs=(any_spec, any_spec),
            scratch_shapes=[
                pltpu.VMEM((N_SLOTS, 2, N_GROUPS, N_CP, G_ROWS, HD), jnp.bfloat16),
                pltpu.VMEM((N_SLOTS, 2, N_HALF, K_LOCAL, HD), jnp.bfloat16),
                pltpu.VMEM((N_SLOTS, N_CP, 8, 128), jnp.float32),
                pltpu.VMEM((N_SLOTS, N_GROUPS, N_HALF, G_ROWS, HD), jnp.float32),
                pltpu.VMEM((N_SLOTS, N_GROUPS, N_CP, G_ROWS, HD), jnp.float32),
                pltpu.VMEM((N_SLOTS, N_GROUPS, N_HALF, G_ROWS, HD), jnp.bfloat16),
                pltpu.VMEM((N_SLOTS, 2, N_HALF, K_LOCAL, HD), jnp.float32),
                pltpu.SemaphoreType.DMA((N_SLOTS, 3)),
                pltpu.SemaphoreType.DMA((N_SLOTS, 3, N_HALF)),
                pltpu.SemaphoreType.DMA((2, N_HALF)),
                pltpu.SemaphoreType.DMA((2, N_SLOTS, 2)),
                pltpu.SemaphoreType.DMA((N_SLOTS, 2, N_HALF)),
                pltpu.SemaphoreType.DMA((2, N_SLOTS)),
                pltpu.SemaphoreType.DMA((2,)),
            ],
            compiler_params=pltpu.CompilerParams(collective_id=0, has_side_effects=True, vmem_limit_bytes=40 * 1024 * 1024),
            name="head_exchange",
        )(qd, kv, stats)

        dq = dq.reshape(N_HEADS, rows, HD).transpose(1, 0, 2).reshape(queries.shape)
        return dq, dkv[:, 0].transpose(1, 0, 2), dkv[:, 1].transpose(1, 0, 2)

    return jax.shard_map(per_device, mesh=mesh, in_specs=(spec_q, spec_kv, spec_kv, spec_q, spec_lse, spec_q), out_specs=(spec_q, spec_kv, spec_kv), check_vma=False)
```

```python
import functools

import jax
import jax.numpy as jnp
from jax import lax
from jax.experimental import pallas as pl
from jax.experimental.pallas import tpu as pltpu
from jax.sharding import PartitionSpec as P

MESH = pl.DeviceIdType.MESH
N_CP = 16
N_HEADS = 26
N_HALF = 8
N_SLOTS = 6
N_GROUPS = 3
G_ROWS = 32
SEG_PER_G = 4
Q_LOCAL = 8
K_LOCAL = 128
HD = 128
SEG_LEN = N_CP * Q_LOCAL
GROUP_Q = N_CP * G_ROWS
KEY_SUPER = 512
SRC_PER_SUPER = KEY_SUPER // K_LOCAL
SUPER_PER_HALF = N_HALF // SRC_PER_SUPER
PREFIX0 = 512
KEY_TILE = 256


def at_end(dev):
    return (dev < 4) | (dev >= 12)


def head_of(slot, dev):
    pos = dev % 4
    return jnp.where(at_end(dev), 22 + pos, jnp.where(slot == 5, 20 + pos // 2, 4 * slot + pos))


def slots_of(dev):
    return jnp.where(at_end(dev), 1, jnp.where(dev % 2 == 0, 6, 5))


def kernel(qd_ref, kv_ref, st_ref, dq_out, dkv_out, q_buf, kv_buf, st_buf, part_buf, dq_acc, dq_stage, dkv_stage, in_sems, send_sems, direct_sems, fwd_sems, ret_sems, part_sems, out_sems):
    me = lax.axis_index("cp")
    my_slots = slots_of(me)
    half = me // N_HALF
    half_dev = half * N_HALF
    partner = (3 - me // 4) * 4 + me % 4
    score_scale = HD ** -0.5

    barrier = pltpu.get_barrier_semaphore()

    def greet(k, carry):
        pl.semaphore_signal(barrier, inc=1, device_id={"cp": lax.rem(me + k, N_CP)}, device_id_type=MESH)
        return carry

    lax.fori_loop(1, N_CP, greet, 0)
    pl.semaphore_wait(barrier, N_CP - 1)

    def in_parts(slot, dev):
        head = head_of(slot, dev)
        return (
            (0, qd_ref.at[head], q_buf.at[slot, :, :, me]),
            (1, kv_ref.at[head], kv_buf.at[slot, :, me % N_HALF]),
            (2, st_ref.at[head], st_buf.at[slot, me]),
        )

    def each_in_copy(slot, act):
        for kinds in ((0, 2), (1,)):

            def one(n, carry):
                dev = half_dev + lax.rem(me + n, N_HALF)

                @pl.when(slot < slots_of(dev))
                def _():
                    parts = in_parts(slot, dev)
                    for kind in kinds:
                        act(pltpu.make_async_remote_copy(
                            src_ref=parts[kind][1], dst_ref=parts[kind][2], send_sem=send_sems.at[slot, kind, dev % N_HALF],
                            recv_sem=in_sems.at[slot, kind], device_id={"cp": dev}, device_id_type=MESH,
                        ))

                return carry

            lax.fori_loop(1, N_HALF, one, 0)

    def each_direct_copy(act):
        for my_half in range(2):

            @pl.when(half == my_half)
            def _():
                first = 1 - my_half

                def one(k, carry):
                    dev = (1 - my_half) * N_HALF + lax.rem(me + k, N_HALF)
                    head = head_of(0, dev)
                    parts = ((qd_ref.at[head, :, first:], q_buf.at[0, :, first:, me]), (st_ref.at[head], st_buf.at[0, me]))
                    for kind, (src, dst) in enumerate(parts):
                        act(pltpu.make_async_remote_copy(
                            src_ref=src, dst_ref=dst, send_sem=direct_sems.at[kind, dev % N_HALF], recv_sem=fwd_sems.at[1, 0, kind],
                            device_id={"cp": dev}, device_id_type=MESH,
                        ))
                    return carry

                lax.fori_loop(0, N_HALF, one, 0)

    for slot in range(N_SLOTS):

        @pl.when(slot < my_slots)
        def _():
            for kind, src, dst in in_parts(slot, me):
                pltpu.make_async_copy(src, dst, in_sems.at[slot, kind]).start()

        if slot == 0:
            each_direct_copy(lambda copy: copy.start())
        each_in_copy(slot, lambda copy: copy.start())

    def slab(slot, of_half):
        first = 1 - of_half
        return q_buf.at[slot, :, first:, of_half * N_HALF:(of_half + 1) * N_HALF]

    def stat_slab(slot, of_half):
        return st_buf.at[slot, of_half * N_HALF:(of_half + 1) * N_HALF]

    def forwards(slot, my_half):
        return [
            pltpu.make_async_remote_copy(
                src_ref=ref, dst_ref=ref, send_sem=fwd_sems.at[0, slot, kind], recv_sem=fwd_sems.at[1, slot, kind],
                device_id={"cp": partner}, device_id_type=MESH,
            )
            for kind, ref in enumerate((slab(slot, my_half), stat_slab(slot, my_half)))
        ]

    def receive(slot):
        own = pl.ds(half_dev, N_HALF)
        for kind, ref in ((0, q_buf.at[slot, :, :, own]), (2, st_buf.at[slot, own])):
            pltpu.make_async_copy(ref, ref, in_sems.at[slot, kind]).wait()
        for my_half in range(2):

            @pl.when((half == my_half) & (slot > 0))
            def _():
                for copy in forwards(slot, my_half):
                    copy.start()

    def receive_forwarded(slot):
        for my_half in range(2):

            @pl.when(half == my_half)
            def _():
                for kind, ref in enumerate((slab(slot, 1 - my_half), stat_slab(slot, 1 - my_half))):
                    pltpu.make_async_copy(ref, ref, fwd_sems.at[1, slot, kind]).wait()

    def dkv_remote(slot, dev):
        return pltpu.make_async_remote_copy(
            src_ref=dkv_stage.at[slot, :, dev % N_HALF], dst_ref=dkv_out.at[head_of(slot, me)], send_sem=ret_sems.at[slot, 1, dev % N_HALF],
            recv_sem=out_sems.at[1], device_id={"cp": dev}, device_id_type=MESH,
        )

    def dq_remote(slot, dev):
        return pltpu.make_async_remote_copy(
            src_ref=dq_stage.at[slot, :, dev % N_HALF], dst_ref=dq_out.at[head_of(slot, me)], send_sem=ret_sems.at[slot, 0, dev % N_HALF],
            recv_sem=out_sems.at[0], device_id={"cp": dev}, device_id_type=MESH,
        )

    def part_remote(slot, my_half):
        first, other = my_half, (1 - my_half) * N_HALF
        return pltpu.make_async_remote_copy(
            src_ref=dq_acc.at[slot, first:, other:other + N_HALF], dst_ref=part_buf.at[slot, first:], send_sem=part_sems.at[0, slot],
            recv_sem=part_sems.at[1, slot], device_id={"cp": partner}, device_id_type=MESH,
        )

    key_iota = lax.broadcasted_iota(jnp.int32, (KEY_TILE, GROUP_Q), 0)
    lane = lax.broadcasted_iota(jnp.int32, (1, GROUP_Q), 1)
    lane_pos = PREFIX0 + (lane % G_ROWS // Q_LOCAL) * SEG_LEN + (lane // G_ROWS) * Q_LOCAL + lane % Q_LOCAL

    def finish_dq(slot):
        for my_half in range(2):

            @pl.when(half == my_half)
            def _():
                arrived = part_buf.at[slot, 1 - my_half:]
                pltpu.make_async_copy(arrived, arrived, part_sems.at[1, slot]).wait()
                own = pl.ds(my_half * N_HALF, N_HALF)
                first = dq_acc[slot, 0, own] if my_half == 0 else part_buf[slot, 0]
                dq_stage[slot, 0] = (first * score_scale).astype(jnp.bfloat16)
                for grp in range(1, N_GROUPS):
                    dq_stage[slot, grp] = ((dq_acc[slot, grp, own] + part_buf[slot, grp]) * score_scale).astype(jnp.bfloat16)

        pltpu.make_async_copy(dq_stage.at[slot, :, me % N_HALF], dq_out.at[head_of(slot, me)], out_sems.at[0]).start()

        def give_dq(k, carry):
            dq_remote(slot, half_dev + lax.rem(me + k, N_HALF)).start()
            return carry

        lax.fori_loop(1, N_HALF, give_dq, 0)

    def run_slot(slot, carry):
        @pl.when((slot > 0) & (slot + 1 < my_slots))
        def _():
            receive(slot + 1)

        receive_forwarded(slot)
        pltpu.make_async_copy(kv_buf.at[slot], kv_buf.at[slot], in_sems.at[slot, 1]).wait()
        dq_acc[slot] = jnp.zeros(dq_acc.shape[1:], jnp.float32)

        def run_super(sup_local, carry):
            sup = half * SUPER_PER_HALF + sup_local
            dkv_stage[slot, :, pl.ds(sup_local * SRC_PER_SUPER, SRC_PER_SUPER)] = jnp.zeros((2, SRC_PER_SUPER, K_LOCAL, HD), jnp.float32)

            def run_group(grp, carry):
                q = q_buf[slot, 0, grp].reshape(GROUP_Q, HD)
                do = q_buf[slot, 1, grp].reshape(GROUP_Q, HD)
                lse_rows, delta_rows = [], []
                for quad in range(N_CP // 4):
                    lse_rows.append(jnp.sum(st_buf[slot, pl.ds(quad * 4, 4), grp], axis=0, keepdims=True))
                    delta_rows.append(jnp.sum(st_buf[slot, pl.ds(quad * 4, 4), N_GROUPS + grp], axis=0, keepdims=True))
                lse = jnp.concatenate(lse_rows, axis=1)
                delta = jnp.concatenate(delta_rows, axis=1)
                q_pos = lane_pos + grp * (SEG_PER_G * SEG_LEN)
                dq_part = jnp.zeros((GROUP_Q, HD), jnp.float32)
                for tile in range(KEY_SUPER // KEY_TILE):
                    per = KEY_TILE // K_LOCAL
                    block = pl.ds(sup_local * SRC_PER_SUPER + tile * per, per)
                    key = kv_buf[slot, 0, block].reshape(KEY_TILE, HD)
                    val = kv_buf[slot, 1, block].reshape(KEY_TILE, HD)
                    causal = key_iota + (sup * KEY_SUPER + tile * KEY_TILE) <= q_pos
                    contract_last = (((1,), (1,)), ((), ()))
                    scores = lax.dot_general(key, q, contract_last, preferred_element_type=jnp.float32) * score_scale
                    weights = jnp.where(causal, jnp.exp(scores - lse), 0.0)
                    grad_p = lax.dot_general(val, do, contract_last, preferred_element_type=jnp.float32)
                    grad_s = (weights * (grad_p - delta)).astype(jnp.bfloat16)
                    part_v = jnp.dot(weights.astype(jnp.bfloat16), do, preferred_element_type=jnp.float32)
                    part_k = jnp.dot(grad_s, q, preferred_element_type=jnp.float32)
                    dkv_stage[slot, 0, block] += (part_k * score_scale).reshape(per, K_LOCAL, HD)
                    dkv_stage[slot, 1, block] += part_v.reshape(per, K_LOCAL, HD)
                    dq_part += lax.dot_general(grad_s, key, (((0,), (0,)), ((), ())), preferred_element_type=jnp.float32)
                dq_acc[slot, grp] += dq_part.reshape(N_CP, G_ROWS, HD)
                return carry

            lax.fori_loop(jnp.maximum(sup - 1, 0), N_GROUPS, run_group, 0)

            def give_back(k, carry):
                dev = half_dev + sup_local * SRC_PER_SUPER + k

                @pl.when(dev != me)
                def _():
                    dkv_remote(slot, dev).start()

                @pl.when(dev == me)
                def _():
                    pltpu.make_async_copy(dkv_stage.at[slot, :, me % N_HALF], dkv_out.at[head_of(slot, me)], out_sems.at[1]).start()

                return carry

            lax.fori_loop(0, SRC_PER_SUPER, give_back, 0)
            return carry

        lax.fori_loop(0, SUPER_PER_HALF, run_super, 0)
        for my_half in range(2):

            @pl.when(half == my_half)
            def _():
                part_remote(slot, my_half).start()

        @pl.when((slot == 0) & (my_slots > 1))
        def _():
            receive(slot + 1)

        @pl.when(slot > 0)
        def _():
            finish_dq(slot - 1)

        return carry

    receive(0)
    lax.fori_loop(0, my_slots, run_slot, 0)
    finish_dq(my_slots - 1)

    for slot in range(N_SLOTS):
        each_in_copy(slot, lambda copy: copy.wait_send())
        if slot == 0:
            each_direct_copy(lambda copy: copy.wait_send())

        @pl.when(slot < my_slots)
        def _():
            def drain(k, carry):
                dev = half_dev + lax.rem(me + k, N_HALF)
                dq_remote(slot, dev).wait_send()
                dkv_remote(slot, dev).wait_send()
                return carry

            lax.fori_loop(1, N_HALF, drain, 0)
            for my_half in range(2):

                @pl.when(half == my_half)
                def _():
                    if slot > 0:
                        for copy in forwards(slot, my_half):
                            copy.wait_send()
                    part_remote(slot, my_half).wait_send()

    pltpu.make_async_copy(dq_out, dq_out, out_sems.at[0]).wait()
    pltpu.make_async_copy(dkv_out, dkv_out, out_sems.at[1]).wait()


def solution(mesh):
    spec_q = P(None, "cp", "heads", None)
    spec_kv = P("cp", "heads", None)
    spec_lse = P(None, "cp", "heads")

    def per_device(queries, key_vecs, value_vecs, attn_out, log_sum_exp, grad_out):
        rows = queries.shape[0] * queries.shape[1]
        row_delta = jnp.sum(grad_out.astype(jnp.float32) * attn_out.astype(jnp.float32), axis=-1)
        by_head = lambda x: x.reshape(rows, N_HEADS, HD).transpose(1, 0, 2).reshape(N_HEADS, N_GROUPS, G_ROWS, HD)
        qd = jnp.stack([by_head(queries), by_head(grad_out)], axis=1)
        kv = jnp.stack([key_vecs.transpose(1, 0, 2), value_vecs.transpose(1, 0, 2)], axis=1)
        stats = jnp.stack([log_sum_exp, row_delta]).reshape(2, N_GROUPS, G_ROWS, N_HEADS).transpose(3, 0, 1, 2).reshape(N_HEADS, 6, 1, G_ROWS)
        quarter = (jnp.arange(4) == lax.axis_index("cp") % 4)[:, None]
        stats = jnp.where(quarter, stats, 0.0).reshape(N_HEADS, 6, 4 * G_ROWS)
        stats = jnp.pad(stats, ((0, 0), (0, 2), (0, 0)))

        any_spec = pl.BlockSpec(memory_space=pl.ANY)
        dq, dkv = pl.pallas_call(
            kernel,
            out_shape=(
                jax.ShapeDtypeStruct((N_HEADS, N_GROUPS, G_ROWS, HD), jnp.bfloat16),
                jax.ShapeDtypeStruct((N_HEADS, 2, K_LOCAL, HD), jnp.float32),
            ),
            in_specs=[any_spec] * 3,
            out_specs=(any_spec, any_spec),
            scratch_shapes=[
                pltpu.VMEM((N_SLOTS, 2, N_GROUPS, N_CP, G_ROWS, HD), jnp.bfloat16),
                pltpu.VMEM((N_SLOTS, 2, N_HALF, K_LOCAL, HD), jnp.bfloat16),
                pltpu.VMEM((N_SLOTS, N_CP, 8, 128), jnp.float32),
                pltpu.VMEM((N_SLOTS, N_GROUPS, N_HALF, G_ROWS, HD), jnp.float32),
                pltpu.VMEM((N_SLOTS, N_GROUPS, N_CP, G_ROWS, HD), jnp.float32),
                pltpu.VMEM((N_SLOTS, N_GROUPS, N_HALF, G_ROWS, HD), jnp.bfloat16),
                pltpu.VMEM((N_SLOTS, 2, N_HALF, K_LOCAL, HD), jnp.float32),
                pltpu.SemaphoreType.DMA((N_SLOTS, 3)),
                pltpu.SemaphoreType.DMA((N_SLOTS, 3, N_HALF)),
                pltpu.SemaphoreType.DMA((2, N_HALF)),
                pltpu.SemaphoreType.DMA((2, N_SLOTS, 2)),
                pltpu.SemaphoreType.DMA((N_SLOTS, 2, N_HALF)),
                pltpu.SemaphoreType.DMA((2, N_SLOTS)),
                pltpu.SemaphoreType.DMA((2,)),
            ],
            compiler_params=pltpu.CompilerParams(collective_id=0, has_side_effects=True, vmem_limit_bytes=40 * 1024 * 1024),
            name="head_exchange",
        )(qd, kv, stats)

        dq = dq.reshape(N_HEADS, rows, HD).transpose(1, 0, 2).reshape(queries.shape)
        return dq, dkv[:, 0].transpose(1, 0, 2), dkv[:, 1].transpose(1, 0, 2)

    return jax.shard_map(per_device, mesh=mesh, in_specs=(spec_q, spec_kv, spec_kv, spec_q, spec_lse, spec_q), out_specs=(spec_q, spec_kv, spec_kv), check_vma=False)
```
